256 devices in a mesh: groups: 4 (over x, y), blk: 64 (over z, core).
Axes of the slice: x: 2, y: 2, z: 32, core: 2. Of those that a mesh axis runs over, the one named last changes fastest.
The devices are a block of a 4x8x32 slice.
Arguments:
- queries: bfloat16 [128, 64, 2048], P('blk', 'groups'), parts along dimension 1, may hold values from -24 to 24
- keys: bfloat16 [524288, 512], P(('groups', 'blk')), parts along dimension 0, may hold values from -24 to 24
- values: bfloat16 [524288, 512], P(('groups', 'blk')), parts along dimension 0, may hold values from -24 to 24
- out_weight: bfloat16 [2048, 2048], replicated, may hold values from -0.125 to 0.125
- chosen: int32 [64, 12], P('groups'), parts along dimension 0, may hold values from 0 to 255, as said below
- tile_start: int32 [64], P('groups'), parts along dimension 0, may hold values from 0 to 130944, as said below
Outputs:
- projected: bfloat16 [128, 64, 2048], P('blk', 'groups'), parts along dimension 1
The draws below stay inside these ranges and needn't reach their ends.
There are 4 independent parts, one for each index of `groups`. The reference program is written for one: setup_inputs(seed, part) draws one part's arguments, and reference() takes and returns one part's arrays. A program takes and returns all parts, laid end to end along the dimension named above; an argument that names none is the same for every part. Nothing has to cross between parts.
Inputs may be any that keep to these rules, and one draw needn't show every extreme that they name: `chosen`: row t lists 12 different blocks; the first is the block that holds tile t's positions, the others lie before it. Each block is listed by at most 2 tiles, and some block by exactly 2. `tile_start[t]` is a multiple of 128; tile t's queries have positions tile_start[t] to tile_start[t] + 127, all inside block chosen[t, 0].
All inputs are finite; a program needn't handle non-finite values.
Results may differ from the reference program's by a relative error of at most 0.0064.
Values may be sent and summed in bfloat16 or wider, within the bound.
A program may use at most 128 MiB of HBM per device.

```python
import math
import jax
import jax.numpy as jnp
from jax import lax

QH = 16
KVH = 4
HD = 128
DOUT = 2048
BLOCK = 512
TILE = 128
TOPK = 12
CAP = 2
NBLK = 256
QTILES = 16
KEYS = 131072


def route_plan(seed_key):
    plan_key = jax.random.fold_in(seed_key, 7)
    low_edge = NBLK - NBLK // 8
    own_order = jax.random.permutation(jax.random.fold_in(plan_key, 1), QTILES)
    own_block = (low_edge + own_order % (NBLK // 8)).astype(jnp.int32)
    offsets = jax.random.randint(jax.random.fold_in(plan_key, 2), (QTILES,), 0, BLOCK // TILE)
    starts = (own_block * BLOCK + offsets * TILE).astype(jnp.int32)
    jitter = jax.random.randint(jax.random.fold_in(plan_key, 3), (QTILES, NBLK), 0, 4096)
    popular = jax.random.randint(jax.random.fold_in(plan_key, 4), (), 0, low_edge)
    block_index = jnp.arange(NBLK, dtype=jnp.int32)

    def pick_blocks(counts, inputs):
        row_jitter, own_one = inputs
        scored = row_jitter * NBLK + block_index + jnp.where(block_index == popular, 8192 * NBLK, 0)
        usable = (block_index < low_edge) & (counts < CAP)
        scored = jnp.where(usable, scored, -1 - block_index)
        ranked, picked = lax.top_k(scored, TOPK - 1)
        counts = counts + jnp.sum((picked[:, None] == block_index[None, :]).astype(jnp.int32), axis=0)
        return (counts, jnp.concatenate([own_one[None], picked.astype(jnp.int32)]))
    counts, chosen = lax.scan(pick_blocks, jnp.zeros((NBLK,), jnp.int32), (jitter, own_block))
    return (chosen, starts)


def draw_queries(key, part):
    result = jnp.clip(2.0 * jax.random.normal(jax.random.fold_in(key, 21), (TILE, QTILES, QH * HD), jnp.float32), -8.0, 8.0)
    return result.astype(jnp.bfloat16)


def draw_keys(key, part):
    result = jnp.clip(jax.random.normal(jax.random.fold_in(key, 22), (KEYS, KVH * HD), jnp.float32), -4.0, 4.0)
    return result.astype(jnp.bfloat16)


def draw_chosen(key, part):
    return route_plan(key)[0]


def draw_tile_start(key, part):
    return route_plan(key)[1]


def levels(stream_key, extent, cuts, low, top_value):
    def one(dim, blocks):
        heights = jax.random.uniform(jax.random.fold_in(jax.random.fold_in(stream_key, 6), dim), (blocks,), jnp.float32, low / len(cuts), top_value / len(cuts))
        return jnp.repeat(jnp.exp(heights), extent[dim] // blocks).reshape((-1,) + (1,) * (len(extent) - dim - 1))

    gain = one(*cuts[0])
    for cut in cuts[1:]:
        gain = gain * one(*cut)
    return gain


def centred(stream_key, dims, scale, most, pieces=(), held_as=jnp.bfloat16):
    values = jax.random.normal(stream_key, dims, jnp.float32) * scale
    if len(pieces) > 0:
        values = levels(stream_key, dims, pieces, -0.22, 0.18) * values
    return jnp.clip(values, min=-most, max=most).astype(held_as)


def setup_inputs(seed: int = 0, part: int = 0) -> dict:
    arg_keys = jax.random.split(jax.random.key(seed), 7)
    own_keys = jax.random.split(jax.random.fold_in(arg_keys[6], part), 7)
    queries = draw_queries(jax.random.fold_in(jax.random.fold_in(arg_keys[6], part), 71), part)
    keys = draw_keys(jax.random.fold_in(jax.random.fold_in(arg_keys[6], part), 71), part)
    values = centred(own_keys[2], (KEYS, KVH * HD), 4.0, 24.0, ((0, 64),))
    out_weight = centred(arg_keys[3], (QH * HD, DOUT), (QH * HD) ** -0.5, 0.125)
    chosen = draw_chosen(jax.random.fold_in(jax.random.fold_in(arg_keys[6], part), 71), part)
    tile_start = draw_tile_start(jax.random.fold_in(jax.random.fold_in(arg_keys[6], part), 71), part)
    return {"queries": queries, "keys": keys, "values": values, "out_weight": out_weight, "chosen": chosen, "tile_start": tile_start}


neg_big = -1e+30

def visit_block(query_tile, tile_begin, block_keys, block_values, block_begin):
    tile_rows = query_tile.shape[0]
    key_count = block_keys.shape[0]
    query_view = query_tile.astype(jnp.float32).reshape(tile_rows, KVH, QH // KVH, HD)
    key_view = block_keys.astype(jnp.float32).reshape(key_count, KVH, HD)
    value_view = block_values.astype(jnp.float32).reshape(key_count, KVH, HD)
    scores = jnp.einsum('rkgd,jkd->kgrj', query_view, key_view) * (1.0 / math.sqrt(HD))
    query_pos = tile_begin + jnp.arange(tile_rows, dtype=jnp.int32)
    key_pos = block_begin + jnp.arange(key_count, dtype=jnp.int32)
    visible = key_pos[None, :] <= query_pos[:, None]
    masked = jnp.where(visible, scores, neg_big)
    highest = lax.optimization_barrier(jnp.max(masked, axis=3, keepdims=True))
    summed = lax.optimization_barrier(jnp.sum(jnp.where(visible, jnp.exp(masked - highest), 0.0), axis=3, keepdims=True))
    log_total = highest + jnp.log(summed)
    weights = jnp.where(visible, jnp.exp(masked - log_total), 0.0).astype(jnp.bfloat16)
    weights = lax.optimization_barrier(weights).astype(jnp.float32)
    partial_value = jnp.einsum('kgrj,jkd->rkgd', weights, value_view)
    partial_value = partial_value.astype(jnp.bfloat16).reshape(tile_rows, QH * HD)
    log_rows = jnp.transpose(log_total[..., 0], (2, 0, 1)).reshape(tile_rows, QH)
    return (partial_value, log_rows)

def reference(queries, keys, values, out_weight, chosen, tile_start):
    tile_view = jnp.transpose(queries, (1, 0, 2))

    def one_tile(inputs):
        query_tile, blocks, tile_begin = inputs

        def one_visit(block_id):
            begin = (block_id * BLOCK).astype(jnp.int32)
            block_keys = lax.dynamic_slice_in_dim(keys, begin, BLOCK, 0)
            block_values = lax.dynamic_slice_in_dim(values, begin, BLOCK, 0)
            return visit_block(query_tile, tile_begin, block_keys, block_values, begin)
        partials, log_rows = lax.map(one_visit, blocks)
        partials = lax.optimization_barrier(partials).astype(jnp.float32)
        highest = lax.optimization_barrier(jnp.max(log_rows, axis=0))
        factor = jnp.exp(log_rows - highest[None])
        numerator = lax.optimization_barrier(jnp.sum(factor[..., None] * partials.reshape(TOPK, TILE, QH, HD), axis=0))
        denominator = lax.optimization_barrier(jnp.sum(factor, axis=0))
        return (numerator / denominator[..., None]).reshape(TILE, QH * HD).astype(jnp.bfloat16)
    merged = lax.map(one_tile, (tile_view, chosen, tile_start))
    merged = jnp.transpose(merged, (1, 0, 2)).reshape(TILE * QTILES, QH * HD)
    result = jnp.dot(merged, out_weight, preferred_element_type=jnp.float32).astype(jnp.bfloat16)
    return result.reshape(TILE, QTILES, DOUT)
```

```python
import functools
import math

import jax
import jax.numpy as jnp
from jax import lax
from jax.experimental import pallas as pl
from jax.experimental.pallas import tpu as pltpu
from jax.sharding import PartitionSpec as P

QH = 16
KVH = 4
GRP = QH // KVH
HD = 128
BLOCK = 512
CAP = 2
PIECES = 2
TERMS = 3
CHUNK_ROWS = 128
VMEM_LIMIT = 60 * 1024 * 1024

MESH = pl.DeviceIdType.MESH
neg_big = -1e30


class Ring:
    def __init__(self, n_dev, cores):
        self.cores = cores
        self.chips = n_dev // cores
        self.ups = self.chips // 2
        self.dns = self.chips - 1 - self.ups
        me = lax.axis_index("blk")
        self.me, self.z, self.core = me, me // cores, me % cores
        self.partner = self.z * cores + (1 - self.core)
        self.above = ((self.z + 1) % self.chips) * cores + self.core
        self.below = ((self.z + self.chips - 1) % self.chips) * cores + self.core

    def greet(self):
        barrier = pltpu.get_barrier_semaphore()
        for target in (self.above, self.below, self.partner):
            pl.semaphore_signal(barrier, inc=1, device_id={"blk": target}, device_id_type=MESH)
        pl.semaphore_wait(barrier, 3)


def remote(src, dst, send_sem, recv_sem, target):
    return pltpu.make_async_remote_copy(
        src_ref=src,
        dst_ref=dst,
        send_sem=send_sem,
        recv_sem=recv_sem,
        device_id={"blk": target},
        device_id_type=MESH,
    )


def send(src, dst, send_sem, recv_sem, target):
    remote(src, dst, send_sem, recv_sem, target).start()


def gather_kernel(
    cores,
    per_device,
    chosen_ref,
    q_hbm,
    all_hbm,
    slot_tab,
    last_tab,
    gath,
    own_sem,
    store_sem,
    ag_up_out,
    ag_up,
    ag_dn_out,
    ag_dn,
    ag_pt_out,
    ag_pt,
):
    n_dev, tiles, _, sub, _ = gath.shape
    slots = per_device * CAP
    group = tiles // PIECES
    topk = chosen_ref.shape[1]
    ring = Ring(n_dev, cores)
    chips, ups, dns, cores = ring.chips, ring.ups, ring.dns, ring.cores
    me, z, core = ring.me, ring.z, ring.core
    above, below, partner = ring.above, ring.below, ring.partner

    def drain(ref, sem):
        remote(ref, ref, sem, sem, partner).wait_recv()

    def gone(ref, sem):
        remote(ref, ref, sem, sem, partner).wait_send()

    own_load = pltpu.make_async_copy(q_hbm, gath.at[me], own_sem)
    own_load.start()
    ring.greet()
    own_load.wait()

    def shard(index, piece):
        return gath.at[index, pl.ds(piece * group, group)]

    def to_partner(index):
        part = gath.at[index]
        send(part, part, ag_pt_out.at[index // cores], ag_pt.at[index // cores], partner)

    def gather_step(step, carry):
        from_below = ((z - step + chips) % chips) * cores + core
        from_above = ((z + step) % chips) * cores + core
        for piece in range(PIECES):
            part = shard(from_below, piece)

            @pl.when(step >= 1)
            def _():
                drain(part, ag_up.at[step - 1, piece])

            send(part, part, ag_up_out.at[step, piece], ag_up.at[step, piece], above)

            @pl.when(step < dns)
            def _():
                other = shard(from_above, piece)

                @pl.when(step >= 1)
                def _():
                    drain(other, ag_dn.at[step - 1, piece])

                send(other, other, ag_dn_out.at[step, piece], ag_dn.at[step, piece], below)

        to_partner(from_below)

        @pl.when((step >= 1) & (step < dns))
        def _():
            to_partner(from_above)

        return carry

    lax.fori_loop(0, ups, gather_step, 0)

    def scan_tile(tile, carry):
        firsts, lasts = carry
        new_firsts, new_lasts = [], []
        for block in range(per_device):
            hit = chosen_ref[tile, 0] == me * per_device + block
            for pick in range(1, topk):
                hit = hit | (chosen_ref[tile, pick] == me * per_device + block)
            fresh = hit & (firsts[block] == tiles)
            new_firsts.append(jnp.where(fresh, tile, firsts[block]))
            new_lasts.append(jnp.where(hit, tile, lasts[block]))
        return tuple(new_firsts), tuple(new_lasts)

    none_yet = (jnp.int32(tiles),) * per_device, (jnp.int32(-1),) * per_device
    firsts, lasts = lax.fori_loop(0, tiles, scan_tile, none_yet)
    slot_tile, slot_live = [], []
    for block in range(per_device):
        live = firsts[block] < tiles
        twice = lasts[block] > firsts[block]
        slot_tile += [jnp.where(live, firsts[block], 0), jnp.where(twice, lasts[block], 0)]
        slot_live += [live, twice]
    for slot in range(slots):
        previous = jnp.int32(slots)
        for before in range(slot):
            same = slot_live[before] & slot_live[slot] & (slot_tile[before] == slot_tile[slot])
            previous = jnp.where(same, before, previous)
        slot_tab[0, slot] = slot_tile[slot]
        slot_tab[1, slot] = jnp.where(slot_live[slot], 1, 0)
        slot_tab[2, slot] = previous
    for tile in range(tiles):
        latest = jnp.int32(slots)
        for slot in range(slots):
            latest = jnp.where(slot_live[slot] & (slot_tile[slot] == tile), slot, latest)
        last_tab[tile] = latest

    from_below = ((z - ups + chips) % chips) * cores + core
    from_above = ((z + dns) % chips) * cores + core
    for piece in range(PIECES):
        drain(shard(from_below, piece), ag_up.at[ups - 1, piece])
    to_partner(from_below)
    for piece in range(PIECES):
        drain(shard(from_above, piece), ag_dn.at[dns - 1, piece])
    to_partner(from_above)

    def partner_shard(chip, carry):
        drain(gath.at[chip * cores + (1 - core)], ag_pt.at[chip])
        for index in (chip * cores + core, chip * cores + (1 - core)):
            pltpu.make_async_copy(gath.at[index], all_hbm.at[index], store_sem.at[index]).start()
        return carry

    lax.fori_loop(0, chips, partner_shard, 0)
    def left(step, carry):
        for piece in range(PIECES):
            gone(shard(((z - step + chips) % chips) * cores + core, piece), ag_up_out.at[step, piece])

            @pl.when(step < dns)
            def _():
                gone(shard(((z + step) % chips) * cores + core, piece), ag_dn_out.at[step, piece])

        return carry

    lax.fori_loop(0, ups, left, 0)

    def left_partner(chip, carry):
        gone(gath.at[chip * cores + core], ag_pt_out.at[chip])
        return carry

    lax.fori_loop(0, chips, left_partner, 0)

    def stored(index, carry):
        pltpu.make_async_copy(gath.at[index], all_hbm.at[index], store_sem.at[index]).wait()
        return carry

    lax.fori_loop(0, n_dev, stored, 0)


def visit_kernel(slot_tab, start_ref, q_ref, k_ref, v_ref, acc, accl):
    slot = pl.program_id(0)
    slots = pl.num_programs(0)
    n_dev, _, _, sub, _ = q_ref.shape
    rows = n_dev * sub
    chunk_rows = min(CHUNK_ROWS, rows)
    chunk_devs = chunk_rows // sub
    chunks = rows // chunk_rows
    per_device = slots // CAP
    block = slot // CAP
    tile = slot_tab[0, slot]
    previous = slot_tab[2, slot]
    offset = start_ref[tile] - (lax.axis_index("blk") * per_device + block) * BLOCK

    @pl.when(slot == 0)
    def _():
        acc[slots] = jnp.zeros(acc.shape[1:], acc.dtype)
        accl[slots] = jnp.full(accl.shape[1:], neg_big, accl.dtype)

    @pl.when(slot_tab[1, slot] > 0)
    def _():
        def visit(chunk, carry):
            devs = pl.ds(chunk * chunk_devs, chunk_devs)
            row = (lax.broadcasted_iota(jnp.int32, (chunk_rows, BLOCK), 0) + chunk * chunk_rows) // GRP
            ahead = lax.broadcasted_iota(jnp.int32, (chunk_rows, BLOCK), 1) - row
            visible = ahead <= offset
            wide = lax.broadcasted_iota(jnp.int32, (chunk_rows, HD), 1) % KVH
            before_lse = accl[previous, devs].reshape(chunk_rows, HD)
            packed = jnp.zeros((chunk_rows, HD), jnp.float32)
            for head in range(KVH):
                query = q_ref[devs, 0, head].astype(jnp.float32)
                query = query.reshape(chunk_rows, HD).astype(jnp.bfloat16)
                key = k_ref[:, head * HD : (head + 1) * HD]
                value = v_ref[:, head * HD : (head + 1) * HD]
                scores = lax.dot_general(
                    query, key, (((1,), (1,)), ((), ())), preferred_element_type=jnp.float32
                ) * (1.0 / math.sqrt(HD))
                scores = jnp.where(visible, scores, neg_big)
                highest = jnp.max(scores, axis=1, keepdims=True)
                weights = jnp.exp(scores - highest)
                total = jnp.sum(weights, axis=1, keepdims=True)
                weights = (weights * (1.0 / total)).astype(jnp.bfloat16)
                partial = jnp.dot(weights, value, preferred_element_type=jnp.float32)
                partial = partial.astype(jnp.bfloat16).astype(jnp.float32)
                lse = highest + jnp.log(total)
                old_lse = before_lse[:, head : head + 1]
                old = acc[previous, devs, head].astype(jnp.float32).reshape(chunk_rows, HD)
                peak = jnp.maximum(lse, old_lse)
                new_part = jnp.exp(lse - peak)
                old_part = jnp.exp(old_lse - peak)
                both = new_part + old_part
                scale = 1.0 / both
                partial = (new_part * scale) * partial + (old_part * scale) * old
                acc[slot, devs, head] = partial.reshape(chunk_devs, sub, HD).astype(jnp.bfloat16)
                packed = jnp.where(wide == head, peak + jnp.log(both), packed)
            accl[slot, devs] = packed.reshape(chunk_devs, sub, HD)
            return carry

        lax.fori_loop(0, chunks, visit, 0)


def scatter_kernel(
    cores,
    tiles,
    last_tab,
    acc,
    accl,
    out_ref,
    upbuf,
    dnbuf,
    psend,
    precv,
    xbuf,
    rs_up_out,
    rs_up,
    rs_dn_out,
    rs_dn,
    rs_pt_out,
    rs_pt,
):
    _, n_dev, _, sub, _ = acc.shape
    group = tiles // PIECES
    ring = Ring(n_dev, cores)
    chips, ups, dns, cores = ring.chips, ring.ups, ring.dns, ring.cores
    me, z, core = ring.me, ring.z, ring.core
    above, below, partner = ring.above, ring.below, ring.partner

    def drain(ref, sem):
        remote(ref, ref, sem, sem, partner).wait_recv()

    def gone(ref, sem):
        remote(ref, ref, sem, sem, partner).wait_send()

    ring.greet()
    lane = lax.broadcasted_iota(jnp.int32, (sub, HD), 1)
    lane_tile = lane // KVH

    def split_lse(value):
        parts = []
        rest = value
        for _ in range(TERMS):
            part = rest.astype(jnp.bfloat16)
            rest = rest - part.astype(jnp.float32)
            parts.append(part)
        return parts

    def store_lse(ref, value):
        for term, part in enumerate(split_lse(value)):
            ref[group * KVH + term] = part

    def read_lse(ref):
        total = ref[group * KVH].astype(jnp.float32)
        for term in range(1, TERMS):
            total = total + ref[group * KVH + term].astype(jnp.float32)
        return total

    empty_lse = jnp.full((sub, HD), neg_big, jnp.float32)
    for ref in (upbuf, dnbuf):
        for piece in range(PIECES):
            ref[0, piece, pl.ds(0, group * KVH)] = jnp.zeros((group * KVH, sub, HD), ref.dtype)
            store_lse(ref.at[0, piece], empty_lse)

    def own_lse(dest, piece):
        value = empty_lse
        for spot in range(group):
            latest = last_tab[piece * group + spot]
            value = jnp.where(lane_tile == spot, accl[latest, dest], value)
        return value

    def own_part(dest, piece, spot, head):
        return acc[last_tab[piece * group + spot], dest, head].astype(jnp.float32)

    def combine(values):
        peak = values[0]
        for value in values[1:]:
            peak = jnp.maximum(peak, value)
        shares = [jnp.exp(value - peak) for value in values]
        total = shares[0]
        for share in shares[1:]:
            total = total + share
        scale = 1.0 / total
        return [share * scale for share in shares], peak + jnp.log(total)

    def blend(refs, dest, piece, shares, spot, head):
        at = spot * KVH + head
        merged = shares[0][:, at : at + 1] * own_part(dest, piece, spot, head)
        for ref, share in zip(refs, shares[1:]):
            merged = merged + share[:, at : at + 1] * ref[at].astype(jnp.float32)
        return merged.astype(jnp.bfloat16)

    def give_partner(place, chip):
        dest = (chip % chips) * cores + (1 - core)
        for piece in range(PIECES):
            store_lse(psend.at[place, piece], own_lse(dest, piece))
            for spot in range(group):
                latest = last_tab[piece * group + spot]
                psend[place, piece, pl.ds(spot * KVH, KVH)] = acc[latest, dest]
        send(psend.at[place], precv.at[place], rs_pt_out.at[place], rs_pt.at[place], partner)

    def give_step(step):
        give_partner(step, z + ups - step)

        @pl.when(step < dns)
        def _():
            give_partner(ups + 1 + step, z + chips - dns + step)

    def hop(buf, step, place, chip, piece, out, recv, target):
        dest = (chip % chips) * cores + core

        @pl.when(step >= 1)
        def _():
            drain(buf.at[step, piece], recv.at[step - 1, piece])

        here = buf.at[step, piece]
        theirs = precv.at[place, piece]
        shares, lse = combine([own_lse(dest, piece), read_lse(here), read_lse(theirs)])
        for spot in range(group):
            for head in range(KVH):
                here[spot * KVH + head] = blend([here, theirs], dest, piece, shares, spot, head)
        store_lse(here, lse)
        send(here, buf.at[step + 1, piece], out.at[step, piece], recv.at[step, piece], target)

    give_step(0)

    def scatter_step(step, carry):
        @pl.when(step + 1 <= ups)
        def _():
            give_step(step + 1)

        drain(precv.at[step], rs_pt.at[step])

        @pl.when(step < dns)
        def _():
            drain(precv.at[ups + 1 + step], rs_pt.at[ups + 1 + step])

        for piece in range(PIECES):
            hop(upbuf, step, step, z + ups - step, piece, rs_up_out, rs_up, above)

            @pl.when(step < dns)
            def _():
                hop(
                    dnbuf,
                    step,
                    ups + 1 + step,
                    z + chips - dns + step,
                    piece,
                    rs_dn_out,
                    rs_dn,
                    below,
                )

        return carry

    lax.fori_loop(0, ups, scatter_step, 0)
    drain(precv.at[ups], rs_pt.at[ups])
    for piece in range(PIECES):
        drain(upbuf.at[ups, piece], rs_up.at[ups - 1, piece])
        drain(dnbuf.at[dns, piece], rs_dn.at[dns - 1, piece])
        refs = [upbuf.at[ups, piece], dnbuf.at[dns, piece], precv.at[ups, piece]]
        shares, _ = combine([own_lse(me, piece)] + [read_lse(ref) for ref in refs])
        for spot in range(group):
            for head in range(KVH):
                base = ((piece * group + spot) * KVH + head) * sub
                merged = blend(refs, me, piece, shares, spot, head)
                xbuf[pl.ds(base, sub)] = merged.astype(jnp.float32)
    for row in range(sub // GRP):
        for head in range(QH):
            first = (head // GRP) * sub + row * GRP + head % GRP
            picked = xbuf[pl.ds(first, tiles, stride=KVH * sub)]
            out_ref[pl.ds(row * tiles, tiles), head * HD : (head + 1) * HD] = picked.astype(
                jnp.bfloat16
            )

    def left(step, carry):
        for piece in range(PIECES):
            gone(upbuf.at[step, piece], rs_up_out.at[step, piece])

            @pl.when(step < dns)
            def _():
                gone(dnbuf.at[step, piece], rs_dn_out.at[step, piece])

        return carry

    lax.fori_loop(0, ups, left, 0)

    def left_partner(chip, carry):
        gone(psend.at[chip], rs_pt_out.at[chip])
        return carry

    lax.fori_loop(0, chips, left_partner, 0)


def on_device(cores, queries, keys, values, out_weight, chosen, tile_start):
    n_dev = lax.axis_size("blk")
    local_rows, tiles, width = queries.shape
    per_device = keys.shape[0] // BLOCK
    slots = per_device * CAP
    sub = local_rows * GRP
    chips = n_dev // cores
    ups = chips // 2
    dns = chips - 1 - ups
    slabs = tiles // PIECES * KVH + TERMS
    shards = queries.reshape(local_rows, tiles, KVH, GRP, HD)
    shards = jnp.transpose(shards, (1, 2, 0, 3, 4)).reshape(tiles, KVH, sub, HD)
    half = jnp.bfloat16
    wide = jnp.float32
    rings = [
        pltpu.SemaphoreType.DMA((ups, PIECES)),
        pltpu.SemaphoreType.DMA((ups, PIECES)),
        pltpu.SemaphoreType.DMA((dns, PIECES)),
        pltpu.SemaphoreType.DMA((dns, PIECES)),
        pltpu.SemaphoreType.DMA((chips,)),
        pltpu.SemaphoreType.DMA((chips,)),
    ]
    in_smem = pl.BlockSpec(memory_space=pltpu.SMEM)
    in_vmem = pl.BlockSpec(memory_space=pltpu.VMEM)
    anywhere = pl.BlockSpec(memory_space=pl.ANY)
    gathered_shape = (n_dev, tiles, KVH, sub, HD)
    gathered, slot_tab, last_tab = pl.pallas_call(
        functools.partial(gather_kernel, cores, per_device),
        out_shape=(
            jax.ShapeDtypeStruct(gathered_shape, half),
            jax.ShapeDtypeStruct((3, slots), jnp.int32),
            jax.ShapeDtypeStruct((tiles,), jnp.int32),
        ),
        in_specs=[in_smem, anywhere],
        out_specs=(anywhere, in_smem, in_smem),
        scratch_shapes=[
            pltpu.VMEM(gathered_shape, half),
            pltpu.SemaphoreType.DMA,
            pltpu.SemaphoreType.DMA((n_dev,)),
        ]
        + rings,
        compiler_params=pltpu.CompilerParams(
            collective_id=0, has_side_effects=True, vmem_limit_bytes=VMEM_LIMIT
        ),
        name="gather_queries",
    )(chosen, shards)
    acc_shape = (slots + 1, n_dev, KVH, sub, HD)
    accl_shape = (slots + 1, n_dev, sub, HD)
    acc, accl = pl.pallas_call(
        visit_kernel,
        out_shape=(
            jax.ShapeDtypeStruct(acc_shape, half),
            jax.ShapeDtypeStruct(accl_shape, wide),
        ),
        grid_spec=pltpu.PrefetchScalarGridSpec(
            num_scalar_prefetch=2,
            grid=(slots,),
            in_specs=[
                pl.BlockSpec((n_dev, 1, KVH, sub, HD), lambda s, tab, start: (0, tab[0, s], 0, 0, 0)),
                pl.BlockSpec((BLOCK, KVH * HD), lambda s, tab, start: (s // CAP, 0)),
                pl.BlockSpec((BLOCK, KVH * HD), lambda s, tab, start: (s // CAP, 0)),
            ],
            out_specs=[
                pl.BlockSpec(acc_shape, lambda s, tab, start: (0, 0, 0, 0, 0)),
                pl.BlockSpec(accl_shape, lambda s, tab, start: (0, 0, 0, 0)),
            ],
        ),
        compiler_params=pltpu.CompilerParams(
            dimension_semantics=("arbitrary",), vmem_limit_bytes=VMEM_LIMIT
        ),
        name="visits",
    )(slot_tab, tile_start, gathered, keys, values)
    merged = pl.pallas_call(
        functools.partial(scatter_kernel, cores, tiles),
        out_shape=jax.ShapeDtypeStruct((local_rows * tiles, width), half),
        in_specs=[in_smem, in_vmem, in_vmem],
        out_specs=in_vmem,
        scratch_shapes=[
            pltpu.VMEM((ups + 1, PIECES, slabs, sub, HD), half),
            pltpu.VMEM((dns + 1, PIECES, slabs, sub, HD), half),
            pltpu.VMEM((chips, PIECES, slabs, sub, HD), half),
            pltpu.VMEM((chips, PIECES, slabs, sub, HD), half),
            pltpu.VMEM((tiles * KVH * sub, HD), wide),
        ]
        + rings,
        compiler_params=pltpu.CompilerParams(
            collective_id=1, has_side_effects=True, vmem_limit_bytes=VMEM_LIMIT
        ),
        name="merge_partials",
    )(last_tab, acc, accl)
    result = jnp.dot(merged, out_weight, preferred_element_type=jnp.float32).astype(jnp.bfloat16)
    return result.reshape(local_rows, tiles, out_weight.shape[1])


def solution(mesh):
    placed = (
        P("blk", "groups", None),
        P(("groups", "blk"), None),
        P(("groups", "blk"), None),
        P(),
        P("groups", None),
        P("groups"),
    )
    return jax.shard_map(
        functools.partial(on_device, 2),
        mesh=mesh,
        in_specs=placed,
        out_specs=P("blk", "groups", None),
        check_vma=False,
    )
```

```python
import functools
import math

import jax
import jax.numpy as jnp
from jax import lax
from jax.experimental import pallas as pl
from jax.experimental.pallas import tpu as pltpu
from jax.sharding import PartitionSpec as P

QH = 16
KVH = 4
GRP = QH // KVH
HD = 128
BLOCK = 512
CAP = 2
PIECES = 4
TERMS = 3
CHUNK_ROWS = 256
VMEM_LIMIT = 60 * 1024 * 1024

MESH = pl.DeviceIdType.MESH
neg_big = -1e30


class Ring:
    def __init__(self, n_dev, cores):
        self.cores = cores
        self.chips = n_dev // cores
        self.ups = self.chips // 2
        self.dns = self.chips - 1 - self.ups
        me = lax.axis_index("blk")
        self.me, self.z, self.core = me, me // cores, me % cores
        self.partner = self.z * cores + (1 - self.core)
        self.above = ((self.z + 1) % self.chips) * cores + self.core
        self.below = ((self.z + self.chips - 1) % self.chips) * cores + self.core

    def greet(self):
        barrier = pltpu.get_barrier_semaphore()
        for target in (self.above, self.below, self.partner):
            pl.semaphore_signal(barrier, inc=1, device_id={"blk": target}, device_id_type=MESH)
        pl.semaphore_wait(barrier, 3)


def remote(src, dst, send_sem, recv_sem, target):
    return pltpu.make_async_remote_copy(
        src_ref=src,
        dst_ref=dst,
        send_sem=send_sem,
        recv_sem=recv_sem,
        device_id={"blk": target},
        device_id_type=MESH,
    )


def send(src, dst, send_sem, recv_sem, target):
    remote(src, dst, send_sem, recv_sem, target).start()


def gather_kernel(
    cores,
    per_device,
    chosen_ref,
    q_hbm,
    all_hbm,
    slot_tab,
    last_tab,
    gath,
    own_sem,
    store_sem,
    ag_up_out,
    ag_up,
    ag_dn_out,
    ag_dn,
    ag_pt_out,
    ag_pt,
):
    n_dev, tiles, _, sub, _ = gath.shape
    slots = per_device * CAP
    group = tiles // PIECES
    topk = chosen_ref.shape[1]
    ring = Ring(n_dev, cores)
    chips, ups, dns, cores = ring.chips, ring.ups, ring.dns, ring.cores
    me, z, core = ring.me, ring.z, ring.core
    above, below, partner = ring.above, ring.below, ring.partner

    def drain(ref, sem):
        remote(ref, ref, sem, sem, partner).wait_recv()

    def gone(ref, sem):
        remote(ref, ref, sem, sem, partner).wait_send()

    own_load = pltpu.make_async_copy(q_hbm, gath.at[me], own_sem)
    own_load.start()
    ring.greet()
    own_load.wait()

    def shard(index, piece):
        return gath.at[index, pl.ds(piece * group, group)]

    def to_partner(index):
        part = gath.at[index]
        send(part, part, ag_pt_out.at[index // cores], ag_pt.at[index // cores], partner)

    def gather_step(step, carry):
        from_below = ((z - step + chips) % chips) * cores + core
        from_above = ((z + step) % chips) * cores + core
        for piece in range(PIECES):
            part = shard(from_below, piece)

            @pl.when(step >= 1)
            def _():
                drain(part, ag_up.at[step - 1, piece])

            send(part, part, ag_up_out.at[step, piece], ag_up.at[step, piece], above)

            @pl.when(step < dns)
            def _():
                other = shard(from_above, piece)

                @pl.when(step >= 1)
                def _():
                    drain(other, ag_dn.at[step - 1, piece])

                send(other, other, ag_dn_out.at[step, piece], ag_dn.at[step, piece], below)

        to_partner(from_below)

        @pl.when((step >= 1) & (step < dns))
        def _():
            to_partner(from_above)

        return carry

    lax.fori_loop(0, ups, gather_step, 0)

    def scan_tile(tile, carry):
        firsts, lasts = carry
        new_firsts, new_lasts = [], []
        for block in range(per_device):
            hit = chosen_ref[tile, 0] == me * per_device + block
            for pick in range(1, topk):
                hit = hit | (chosen_ref[tile, pick] == me * per_device + block)
            fresh = hit & (firsts[block] == tiles)
            new_firsts.append(jnp.where(fresh, tile, firsts[block]))
            new_lasts.append(jnp.where(hit, tile, lasts[block]))
        return tuple(new_firsts), tuple(new_lasts)

    none_yet = (jnp.int32(tiles),) * per_device, (jnp.int32(-1),) * per_device
    firsts, lasts = lax.fori_loop(0, tiles, scan_tile, none_yet)
    slot_tile, slot_live = [], []
    for block in range(per_device):
        live = firsts[block] < tiles
        twice = lasts[block] > firsts[block]
        slot_tile += [jnp.where(live, firsts[block], 0), jnp.where(twice, lasts[block], 0)]
        slot_live += [live, twice]
    for slot in range(slots):
        previous = jnp.int32(slots)
        for before in range(slot):
            same = slot_live[before] & slot_live[slot] & (slot_tile[before] == slot_tile[slot])
            previous = jnp.where(same, before, previous)
        slot_tab[0, slot] = slot_tile[slot]
        slot_tab[1, slot] = jnp.where(slot_live[slot], 1, 0)
        slot_tab[2, slot] = previous
    for tile in range(tiles):
        latest = jnp.int32(slots)
        for slot in range(slots):
            latest = jnp.where(slot_live[slot] & (slot_tile[slot] == tile), slot, latest)
        last_tab[tile] = latest

    from_below = ((z - ups + chips) % chips) * cores + core
    from_above = ((z + dns) % chips) * cores + core
    for piece in range(PIECES):
        drain(shard(from_below, piece), ag_up.at[ups - 1, piece])
    to_partner(from_below)
    for piece in range(PIECES):
        drain(shard(from_above, piece), ag_dn.at[dns - 1, piece])
    to_partner(from_above)

    def partner_shard(chip, carry):
        drain(gath.at[chip * cores + (1 - core)], ag_pt.at[chip])
        for index in (chip * cores + core, chip * cores + (1 - core)):
            pltpu.make_async_copy(gath.at[index], all_hbm.at[index], store_sem.at[index]).start()
        return carry

    lax.fori_loop(0, chips, partner_shard, 0)
    def left(step, carry):
        for piece in range(PIECES):
            gone(shard(((z - step + chips) % chips) * cores + core, piece), ag_up_out.at[step, piece])

            @pl.when(step < dns)
            def _():
                gone(shard(((z + step) % chips) * cores + core, piece), ag_dn_out.at[step, piece])

        return carry

    lax.fori_loop(0, ups, left, 0)

    def left_partner(chip, carry):
        gone(gath.at[chip * cores + core], ag_pt_out.at[chip])
        return carry

    lax.fori_loop(0, chips, left_partner, 0)

    def stored(index, carry):
        pltpu.make_async_copy(gath.at[index], all_hbm.at[index], store_sem.at[index]).wait()
        return carry

    lax.fori_loop(0, n_dev, stored, 0)


def visit_kernel(slot_tab, start_ref, q_ref, k_ref, v_ref, acc, accl):
    slot = pl.program_id(0)
    slots = pl.num_programs(0)
    n_dev, _, _, sub, _ = q_ref.shape
    rows = n_dev * sub
    chunk_rows = min(CHUNK_ROWS, rows)
    chunk_devs = chunk_rows // sub
    chunks = rows // chunk_rows
    per_device = slots // CAP
    block = slot // CAP
    tile = slot_tab[0, slot]
    previous = slot_tab[2, slot]
    offset = start_ref[tile] - (lax.axis_index("blk") * per_device + block) * BLOCK

    @pl.when(slot == 0)
    def _():
        acc[slots] = jnp.zeros(acc.shape[1:], acc.dtype)
        accl[slots] = jnp.full(accl.shape[1:], neg_big, accl.dtype)

    @pl.when(slot_tab[1, slot] > 0)
    def _():
        def visit(chunk, masked):
            devs = pl.ds(chunk * chunk_devs, chunk_devs)
            if masked:
                row = lax.broadcasted_iota(jnp.int32, (chunk_rows, BLOCK), 0) + chunk * chunk_rows
                ahead = lax.broadcasted_iota(jnp.int32, (chunk_rows, BLOCK), 1) - row // GRP
                visible = ahead <= offset
            wide = lax.broadcasted_iota(jnp.int32, (chunk_rows, HD), 1) % KVH
            before_lse = accl[previous, devs].reshape(chunk_rows, HD)
            packed = jnp.zeros((chunk_rows, HD), jnp.float32)
            for head in range(KVH):
                query = q_ref[devs, 0, head].astype(jnp.float32)
                query = query.reshape(chunk_rows, HD).astype(jnp.bfloat16)
                key = k_ref[:, head * HD : (head + 1) * HD]
                value = v_ref[:, head * HD : (head + 1) * HD]
                scores = lax.dot_general(
                    query, key, (((1,), (1,)), ((), ())), preferred_element_type=jnp.float32
                )
                if masked:
                    scores = jnp.where(visible, scores, neg_big)
                highest = jnp.max(scores, axis=1, keepdims=True)
                weights = jnp.exp2((scores - highest) * (math.log2(math.e) / math.sqrt(HD)))
                total = jnp.sum(weights, axis=1, keepdims=True)
                weights = (weights * (1.0 / total)).astype(jnp.bfloat16)
                partial = jnp.dot(weights, value, preferred_element_type=jnp.float32)
                partial = partial.astype(jnp.bfloat16).astype(jnp.float32)
                lse = highest * (1.0 / math.sqrt(HD)) + jnp.log(total)
                old_lse = before_lse[:, head : head + 1]
                old = acc[previous, devs, head].astype(jnp.float32).reshape(chunk_rows, HD)
                peak = jnp.maximum(lse, old_lse)
                new_part = jnp.exp(lse - peak)
                old_part = jnp.exp(old_lse - peak)
                both = new_part + old_part
                scale = 1.0 / both
                partial = (new_part * scale) * partial + (old_part * scale) * old
                acc[slot, devs, head] = partial.reshape(chunk_devs, sub, HD).astype(jnp.bfloat16)
                packed = jnp.where(wide == head, peak + jnp.log(both), packed)
            accl[slot, devs] = packed.reshape(chunk_devs, sub, HD)

        def visits(masked):
            def step(chunk, carry):
                visit(chunk, masked)
                return carry

            lax.fori_loop(0, chunks, step, 0)

        pl.when(offset >= BLOCK - 1)(lambda: visits(False))
        pl.when(offset < BLOCK - 1)(lambda: visits(True))


def scatter_kernel(
    cores,
    tiles,
    last_tab,
    acc,
    accl,
    out_ref,
    upbuf,
    dnbuf,
    psend,
    precv,
    xbuf,
    rs_up_out,
    rs_up,
    rs_dn_out,
    rs_dn,
    rs_pt_out,
    rs_pt,
):
    _, n_dev, _, sub, _ = acc.shape
    group = tiles // PIECES
    ring = Ring(n_dev, cores)
    chips, ups, dns, cores = ring.chips, ring.ups, ring.dns, ring.cores
    me, z, core = ring.me, ring.z, ring.core
    above, below, partner = ring.above, ring.below, ring.partner

    def drain(ref, sem):
        remote(ref, ref, sem, sem, partner).wait_recv()

    def gone(ref, sem):
        remote(ref, ref, sem, sem, partner).wait_send()

    ring.greet()
    lane = lax.broadcasted_iota(jnp.int32, (sub, HD), 1)
    width = group * KVH
    lane_tile = (lane % width) // KVH

    def store_lse(ref, value):
        packed = jnp.zeros_like(value)
        rest = value
        for term in range(TERMS):
            part = rest.astype(jnp.bfloat16).astype(jnp.float32)
            rest = rest - part
            here = (lane >= term * width) & (lane < (term + 1) * width)
            packed = jnp.where(here, pltpu.roll(part, term * width, 1) if term else part, packed)
        ref[group * KVH] = packed.astype(jnp.bfloat16)

    def read_lse(ref):
        packed = ref[group * KVH].astype(jnp.float32)
        total = packed
        for term in range(1, TERMS):
            total = total + pltpu.roll(packed, HD - term * width, 1)
        return total

    empty_lse = jnp.full((sub, HD), neg_big, jnp.float32)
    for ref in (upbuf, dnbuf):
        for piece in range(PIECES):
            ref[0, piece, pl.ds(0, group * KVH)] = jnp.zeros((group * KVH, sub, HD), ref.dtype)
            store_lse(ref.at[0, piece], empty_lse)

    def own_lse(dest, piece):
        value = empty_lse
        for spot in range(group):
            latest = last_tab[piece * group + spot]
            value = jnp.where(lane_tile == spot, accl[latest, dest], value)
        return value

    def own_part(dest, piece, spot, head):
        return acc[last_tab[piece * group + spot], dest, head].astype(jnp.float32)

    def combine(values):
        peak = values[0]
        for value in values[1:]:
            peak = jnp.maximum(peak, value)
        shares = [jnp.exp(value - peak) for value in values]
        total = shares[0]
        for share in shares[1:]:
            total = total + share
        scale = 1.0 / total
        return [share * scale for share in shares], peak + jnp.log(total)

    def blend(refs, dest, piece, shares, spot, head):
        at = spot * KVH + head
        merged = shares[0][:, at : at + 1] * own_part(dest, piece, spot, head)
        for ref, share in zip(refs, shares[1:]):
            merged = merged + share[:, at : at + 1] * ref[at].astype(jnp.float32)
        return merged.astype(jnp.bfloat16)

    def give_partner(place, chip):
        dest = (chip % chips) * cores + (1 - core)
        for piece in range(PIECES):
            store_lse(psend.at[place, piece], own_lse(dest, piece))
            for spot in range(group):
                latest = last_tab[piece * group + spot]
                psend[place, piece, pl.ds(spot * KVH, KVH)] = acc[latest, dest]
        send(psend.at[place], precv.at[place], rs_pt_out.at[place], rs_pt.at[place], partner)

    def give_step(step):
        give_partner(step, z + ups - step)

        @pl.when(step < dns)
        def _():
            give_partner(ups + 1 + step, z + chips - dns + step)

    def hop(buf, step, place, chip, piece, out, recv, target):
        dest = (chip % chips) * cores + core

        @pl.when(step >= 1)
        def _():
            drain(buf.at[step, piece], recv.at[step - 1, piece])

        here = buf.at[step, piece]
        theirs = precv.at[place, piece]
        shares, lse = combine([own_lse(dest, piece), read_lse(here), read_lse(theirs)])
        for spot in range(group):
            for head in range(KVH):
                here[spot * KVH + head] = blend([here, theirs], dest, piece, shares, spot, head)
        store_lse(here, lse)
        send(here, buf.at[step + 1, piece], out.at[step, piece], recv.at[step, piece], target)

    give_step(0)

    def scatter_step(step, carry):
        @pl.when(step + 1 <= ups)
        def _():
            give_step(step + 1)

        drain(precv.at[step], rs_pt.at[step])

        @pl.when(step < dns)
        def _():
            drain(precv.at[ups + 1 + step], rs_pt.at[ups + 1 + step])

        for piece in range(PIECES):
            hop(upbuf, step, step, z + ups - step, piece, rs_up_out, rs_up, above)

            @pl.when(step < dns)
            def _():
                hop(
                    dnbuf,
                    step,
                    ups + 1 + step,
                    z + chips - dns + step,
                    piece,
                    rs_dn_out,
                    rs_dn,
                    below,
                )

        return carry

    lax.fori_loop(0, ups, scatter_step, 0)
    drain(precv.at[ups], rs_pt.at[ups])
    for piece in range(PIECES):
        drain(upbuf.at[ups, piece], rs_up.at[ups - 1, piece])
        drain(dnbuf.at[dns, piece], rs_dn.at[dns - 1, piece])
        refs = [upbuf.at[ups, piece], dnbuf.at[dns, piece], precv.at[ups, piece]]
        shares, _ = combine([own_lse(me, piece)] + [read_lse(ref) for ref in refs])
        for spot in range(group):
            for head in range(KVH):
                base = ((piece * group + spot) * KVH + head) * sub
                merged = blend(refs, me, piece, shares, spot, head)
                xbuf[pl.ds(base, sub)] = merged.astype(jnp.float32)
    for row in range(sub // GRP):
        for head in range(QH):
            first = (head // GRP) * sub + row * GRP + head % GRP
            picked = xbuf[pl.ds(first, tiles, stride=KVH * sub)]
            out_ref[pl.ds(row * tiles, tiles), head * HD : (head + 1) * HD] = picked.astype(
                jnp.bfloat16
            )

    def left(step, carry):
        for piece in range(PIECES):
            gone(upbuf.at[step, piece], rs_up_out.at[step, piece])

            @pl.when(step < dns)
            def _():
                gone(dnbuf.at[step, piece], rs_dn_out.at[step, piece])

        return carry

    lax.fori_loop(0, ups, left, 0)

    def left_partner(chip, carry):
        gone(psend.at[chip], rs_pt_out.at[chip])
        return carry

    lax.fori_loop(0, chips, left_partner, 0)


def on_device(cores, queries, keys, values, out_weight, chosen, tile_start):
    n_dev = lax.axis_size("blk")
    local_rows, tiles, width = queries.shape
    per_device = keys.shape[0] // BLOCK
    slots = per_device * CAP
    sub = local_rows * GRP
    chips = n_dev // cores
    ups = chips // 2
    dns = chips - 1 - ups
    slabs = tiles // PIECES * KVH + 1
    shards = queries.reshape(local_rows, tiles, KVH, GRP, HD)
    shards = jnp.transpose(shards, (1, 2, 0, 3, 4)).reshape(tiles, KVH, sub, HD)
    half = jnp.bfloat16
    wide = jnp.float32
    rings = [
        pltpu.SemaphoreType.DMA((ups, PIECES)),
        pltpu.SemaphoreType.DMA((ups, PIECES)),
        pltpu.SemaphoreType.DMA((dns, PIECES)),
        pltpu.SemaphoreType.DMA((dns, PIECES)),
        pltpu.SemaphoreType.DMA((chips,)),
        pltpu.SemaphoreType.DMA((chips,)),
    ]
    in_smem = pl.BlockSpec(memory_space=pltpu.SMEM)
    in_vmem = pl.BlockSpec(memory_space=pltpu.VMEM)
    anywhere = pl.BlockSpec(memory_space=pl.ANY)
    gathered_shape = (n_dev, tiles, KVH, sub, HD)
    gathered, slot_tab, last_tab = pl.pallas_call(
        functools.partial(gather_kernel, cores, per_device),
        out_shape=(
            jax.ShapeDtypeStruct(gathered_shape, half),
            jax.ShapeDtypeStruct((3, slots), jnp.int32),
            jax.ShapeDtypeStruct((tiles,), jnp.int32),
        ),
        in_specs=[in_smem, anywhere],
        out_specs=(anywhere, in_smem, in_smem),
        scratch_shapes=[
            pltpu.VMEM(gathered_shape, half),
            pltpu.SemaphoreType.DMA,
            pltpu.SemaphoreType.DMA((n_dev,)),
        ]
        + rings,
        compiler_params=pltpu.CompilerParams(
            collective_id=0, has_side_effects=True, vmem_limit_bytes=VMEM_LIMIT
        ),
        name="gather_queries",
    )(chosen, shards)
    acc_shape = (slots + 1, n_dev, KVH, sub, HD)
    accl_shape = (slots + 1, n_dev, sub, HD)
    acc, accl = pl.pallas_call(
        visit_kernel,
        out_shape=(
            jax.ShapeDtypeStruct(acc_shape, half),
            jax.ShapeDtypeStruct(accl_shape, wide),
        ),
        grid_spec=pltpu.PrefetchScalarGridSpec(
            num_scalar_prefetch=2,
            grid=(slots,),
            in_specs=[
                pl.BlockSpec((n_dev, 1, KVH, sub, HD), lambda s, tab, start: (0, tab[0, s], 0, 0, 0)),
                pl.BlockSpec((BLOCK, KVH * HD), lambda s, tab, start: (s // CAP, 0)),
                pl.BlockSpec((BLOCK, KVH * HD), lambda s, tab, start: (s // CAP, 0)),
            ],
            out_specs=[
                pl.BlockSpec(acc_shape, lambda s, tab, start: (0, 0, 0, 0, 0)),
                pl.BlockSpec(accl_shape, lambda s, tab, start: (0, 0, 0, 0)),
            ],
        ),
        compiler_params=pltpu.CompilerParams(
            dimension_semantics=("arbitrary",), vmem_limit_bytes=VMEM_LIMIT
        ),
        name="visits",
    )(slot_tab, tile_start, gathered, keys, values)
    merged = pl.pallas_call(
        functools.partial(scatter_kernel, cores, tiles),
        out_shape=jax.ShapeDtypeStruct((local_rows * tiles, width), half),
        in_specs=[in_smem, in_vmem, in_vmem],
        out_specs=in_vmem,
        scratch_shapes=[
            pltpu.VMEM((ups + 1, PIECES, slabs, sub, HD), half),
            pltpu.VMEM((dns + 1, PIECES, slabs, sub, HD), half),
            pltpu.VMEM((chips, PIECES, slabs, sub, HD), half),
            pltpu.VMEM((chips, PIECES, slabs, sub, HD), half),
            pltpu.VMEM((tiles * KVH * sub, HD), wide),
        ]
        + rings,
        compiler_params=pltpu.CompilerParams(
            collective_id=1, has_side_effects=True, vmem_limit_bytes=VMEM_LIMIT
        ),
        name="merge_partials",
    )(last_tab, acc, accl)
    result = jnp.dot(merged, out_weight, preferred_element_type=jnp.float32).astype(jnp.bfloat16)
    return result.reshape(local_rows, tiles, out_weight.shape[1])


def solution(mesh):
    placed = (
        P("blk", "groups", None),
        P(("groups", "blk"), None),
        P(("groups", "blk"), None),
        P(),
        P("groups", None),
        P("groups"),
    )
    return jax.shard_map(
        functools.partial(on_device, 2),
        mesh=mesh,
        in_specs=placed,
        out_specs=P("blk", "groups", None),
        check_vma=False,
    )
```

```python
import functools
import math

import jax
import jax.numpy as jnp
from jax import lax
from jax.experimental import pallas as pl
from jax.experimental.pallas import tpu as pltpu
from jax.sharding import PartitionSpec as P

QH = 16
KVH = 4
GRP = QH // KVH
HD = 128
BLOCK = 512
CAP = 2
PIECES = 4
SHARD_PIECES = 8
TERMS = 3
CHUNK_ROWS = 256
VMEM_LIMIT = 60 * 1024 * 1024

MESH = pl.DeviceIdType.MESH
neg_big = -1e30


class Ring:
    def __init__(self, n_dev, cores):
        self.cores = cores
        self.chips = n_dev // cores
        self.ups = self.chips // 2
        self.dns = self.chips - 1 - self.ups
        me = lax.axis_index("blk")
        self.me, self.z, self.core = me, me // cores, me % cores
        self.partner = self.z * cores + (1 - self.core)
        self.above = ((self.z + 1) % self.chips) * cores + self.core
        self.below = ((self.z + self.chips - 1) % self.chips) * cores + self.core

    def greet(self):
        barrier = pltpu.get_barrier_semaphore()
        for target in (self.above, self.below, self.partner):
            pl.semaphore_signal(barrier, inc=1, device_id={"blk": target}, device_id_type=MESH)
        pl.semaphore_wait(barrier, 3)


def remote(src, dst, send_sem, recv_sem, target):
    return pltpu.make_async_remote_copy(
        src_ref=src,
        dst_ref=dst,
        send_sem=send_sem,
        recv_sem=recv_sem,
        device_id={"blk": target},
        device_id_type=MESH,
    )


def send(src, dst, send_sem, recv_sem, target):
    remote(src, dst, send_sem, recv_sem, target).start()


def gather_kernel(
    cores,
    per_device,
    chosen_ref,
    q_hbm,
    all_hbm,
    slot_tab,
    last_tab,
    gath,
    own_sem,
    store_sem,
    ag_up_out,
    ag_up,
    ag_dn_out,
    ag_dn,
    ag_pt_out,
    ag_pt,
):
    n_dev, tiles, _, sub, _ = gath.shape
    slots = per_device * CAP
    group = tiles // SHARD_PIECES
    topk = chosen_ref.shape[1]
    ring = Ring(n_dev, cores)
    chips, ups, dns, cores = ring.chips, ring.ups, ring.dns, ring.cores
    me, z, core = ring.me, ring.z, ring.core
    above, below, partner = ring.above, ring.below, ring.partner

    def drain(ref, sem):
        remote(ref, ref, sem, sem, partner).wait_recv()

    def gone(ref, sem):
        remote(ref, ref, sem, sem, partner).wait_send()

    own_load = pltpu.make_async_copy(q_hbm, gath.at[me], own_sem)
    own_load.start()
    ring.greet()
    own_load.wait()

    def shard(index, piece):
        return gath.at[index, pl.ds(piece * group, group)]

    def to_partner(index):
        part = gath.at[index]
        send(part, part, ag_pt_out.at[index // cores], ag_pt.at[index // cores], partner)
        pltpu.make_async_copy(part, all_hbm.at[index], store_sem.at[index]).start()

    def gather_step(step, carry):
        from_below = ((z - step + chips) % chips) * cores + core
        from_above = ((z + step) % chips) * cores + core
        for piece in range(SHARD_PIECES):
            part = shard(from_below, piece)

            @pl.when(step >= 1)
            def _():
                drain(part, ag_up.at[step - 1, piece])

            send(part, part, ag_up_out.at[step, piece], ag_up.at[step, piece], above)

            @pl.when(step < dns)
            def _():
                other = shard(from_above, piece)

                @pl.when(step >= 1)
                def _():
                    drain(other, ag_dn.at[step - 1, piece])

                send(other, other, ag_dn_out.at[step, piece], ag_dn.at[step, piece], below)

        to_partner(from_below)

        @pl.when((step >= 1) & (step < dns))
        def _():
            to_partner(from_above)

        return carry

    lax.fori_loop(0, ups, gather_step, 0)

    def scan_tile(tile, carry):
        firsts, lasts = carry
        new_firsts, new_lasts = [], []
        for block in range(per_device):
            hit = chosen_ref[tile, 0] == me * per_device + block
            for pick in range(1, topk):
                hit = hit | (chosen_ref[tile, pick] == me * per_device + block)
            fresh = hit & (firsts[block] == tiles)
            new_firsts.append(jnp.where(fresh, tile, firsts[block]))
            new_lasts.append(jnp.where(hit, tile, lasts[block]))
        return tuple(new_firsts), tuple(new_lasts)

    none_yet = (jnp.int32(tiles),) * per_device, (jnp.int32(-1),) * per_device
    firsts, lasts = lax.fori_loop(0, tiles, scan_tile, none_yet)
    slot_tile, slot_live = [], []
    for block in range(per_device):
        live = firsts[block] < tiles
        twice = lasts[block] > firsts[block]
        slot_tile += [jnp.where(live, firsts[block], 0), jnp.where(twice, lasts[block], 0)]
        slot_live += [live, twice]
    for slot in range(slots):
        previous = jnp.int32(slots)
        for before in range(slot):
            same = slot_live[before] & slot_live[slot] & (slot_tile[before] == slot_tile[slot])
            previous = jnp.where(same, before, previous)
        slot_tab[0, slot] = slot_tile[slot]
        slot_tab[1, slot] = jnp.where(slot_live[slot], 1, 0)
        slot_tab[2, slot] = previous
    for tile in range(tiles):
        latest = jnp.int32(slots)
        for slot in range(slots):
            latest = jnp.where(slot_live[slot] & (slot_tile[slot] == tile), slot, latest)
        last_tab[tile] = latest

    from_below = ((z - ups + chips) % chips) * cores + core
    from_above = ((z + dns) % chips) * cores + core
    for piece in range(SHARD_PIECES):
        drain(shard(from_below, piece), ag_up.at[ups - 1, piece])
    to_partner(from_below)
    for piece in range(SHARD_PIECES):
        drain(shard(from_above, piece), ag_dn.at[dns - 1, piece])
    to_partner(from_above)

    def partner_shard(chip, carry):
        drain(gath.at[chip * cores + (1 - core)], ag_pt.at[chip])
        index = chip * cores + (1 - core)
        pltpu.make_async_copy(gath.at[index], all_hbm.at[index], store_sem.at[index]).start()
        return carry

    lax.fori_loop(0, chips, partner_shard, 0)
    def left(step, carry):
        for piece in range(SHARD_PIECES):
            gone(shard(((z - step + chips) % chips) * cores + core, piece), ag_up_out.at[step, piece])

            @pl.when(step < dns)
            def _():
                gone(shard(((z + step) % chips) * cores + core, piece), ag_dn_out.at[step, piece])

        return carry

    lax.fori_loop(0, ups, left, 0)

    def left_partner(chip, carry):
        gone(gath.at[chip * cores + core], ag_pt_out.at[chip])
        return carry

    lax.fori_loop(0, chips, left_partner, 0)

    def stored(index, carry):
        pltpu.make_async_copy(gath.at[index], all_hbm.at[index], store_sem.at[index]).wait()
        return carry

    lax.fori_loop(0, n_dev, stored, 0)


def visit_kernel(slot_tab, start_ref, q_ref, k_ref, v_ref, acc, accl):
    slot = pl.program_id(0)
    slots = pl.num_programs(0)
    n_dev, _, _, sub, _ = q_ref.shape
    rows = n_dev * sub
    chunk_rows = min(CHUNK_ROWS, rows)
    chunk_devs = chunk_rows // sub
    chunks = rows // chunk_rows
    per_device = slots // CAP
    block = slot // CAP
    tile = slot_tab[0, slot]
    previous = slot_tab[2, slot]
    offset = start_ref[tile] - (lax.axis_index("blk") * per_device + block) * BLOCK

    @pl.when(slot == 0)
    def _():
        acc[slots] = jnp.zeros(acc.shape[1:], acc.dtype)
        accl[slots] = jnp.full(accl.shape[1:], neg_big, accl.dtype)

    @pl.when(slot_tab[1, slot] > 0)
    def _():
        def visit(chunk, masked):
            devs = pl.ds(chunk * chunk_devs, chunk_devs)
            if masked:
                row = lax.broadcasted_iota(jnp.int32, (chunk_rows, BLOCK), 0) + chunk * chunk_rows
                ahead = lax.broadcasted_iota(jnp.int32, (chunk_rows, BLOCK), 1) - row // GRP
                visible = ahead <= offset
            wide = lax.broadcasted_iota(jnp.int32, (chunk_rows, HD), 1) % KVH
            before_lse = accl[previous, devs].reshape(chunk_rows, HD)
            packed = jnp.zeros((chunk_rows, HD), jnp.float32)
            olds = [acc[previous, devs, head] for head in range(KVH)]
            partials = []
            for head in range(KVH):
                query = q_ref[devs, 0, head].astype(jnp.float32)
                query = query.reshape(chunk_rows, HD).astype(jnp.bfloat16)
                key = k_ref[:, head * HD : (head + 1) * HD]
                value = v_ref[:, head * HD : (head + 1) * HD]
                scores = lax.dot_general(
                    query, key, (((1,), (1,)), ((), ())), preferred_element_type=jnp.float32
                )
                if masked:
                    scores = jnp.where(visible, scores, neg_big)
                highest = jnp.max(scores, axis=1, keepdims=True)
                weights = jnp.exp2((scores - highest) * (math.log2(math.e) / math.sqrt(HD)))
                total = jnp.sum(weights, axis=1, keepdims=True)
                weights = (weights * (1.0 / total)).astype(jnp.bfloat16)
                partial = jnp.dot(weights, value, preferred_element_type=jnp.float32)
                partial = partial.astype(jnp.bfloat16).astype(jnp.float32)
                lse = highest * (1.0 / math.sqrt(HD)) + jnp.log(total)
                old_lse = before_lse[:, head : head + 1]
                old = olds[head].astype(jnp.float32).reshape(chunk_rows, HD)
                peak = jnp.maximum(lse, old_lse)
                new_part = jnp.exp(lse - peak)
                old_part = jnp.exp(old_lse - peak)
                both = new_part + old_part
                scale = 1.0 / both
                partial = (new_part * scale) * partial + (old_part * scale) * old
                partials.append(partial.reshape(chunk_devs, sub, HD).astype(jnp.bfloat16))
                packed = jnp.where(wide == head, peak + jnp.log(both), packed)
            for head in range(KVH):
                acc[slot, devs, head] = partials[head]
            accl[slot, devs] = packed.reshape(chunk_devs, sub, HD)

        def visits(masked):
            def step(chunk, carry):
                visit(chunk, masked)
                return carry

            lax.fori_loop(0, chunks, step, 0)

        pl.when(offset >= BLOCK - 1)(lambda: visits(False))
        pl.when(offset < BLOCK - 1)(lambda: visits(True))


def scatter_kernel(
    cores,
    tiles,
    last_tab,
    acc,
    accl,
    out_ref,
    upbuf,
    dnbuf,
    psend,
    precv,
    xbuf,
    rs_up_out,
    rs_up,
    rs_dn_out,
    rs_dn,
    rs_pt_out,
    rs_pt,
):
    _, n_dev, _, sub, _ = acc.shape
    group = tiles // PIECES
    ring = Ring(n_dev, cores)
    chips, ups, dns, cores = ring.chips, ring.ups, ring.dns, ring.cores
    me, z, core = ring.me, ring.z, ring.core
    above, below, partner = ring.above, ring.below, ring.partner

    def drain(ref, sem):
        remote(ref, ref, sem, sem, partner).wait_recv()

    def gone(ref, sem):
        remote(ref, ref, sem, sem, partner).wait_send()

    ring.greet()
    lane = lax.broadcasted_iota(jnp.int32, (sub, HD), 1)
    width = group * KVH
    lane_tile = (lane % width) // KVH

    def store_lse(ref, value):
        packed = jnp.zeros_like(value)
        rest = value
        for term in range(TERMS):
            part = rest.astype(jnp.bfloat16).astype(jnp.float32)
            rest = rest - part
            here = (lane >= term * width) & (lane < (term + 1) * width)
            packed = jnp.where(here, pltpu.roll(part, term * width, 1) if term else part, packed)
        ref[group * KVH] = packed.astype(jnp.bfloat16)

    def read_lse(ref):
        packed = ref[group * KVH].astype(jnp.float32)
        total = packed
        for term in range(1, TERMS):
            total = total + pltpu.roll(packed, HD - term * width, 1)
        return total

    empty_lse = jnp.full((sub, HD), neg_big, jnp.float32)
    for ref in (upbuf, dnbuf):
        for piece in range(PIECES):
            ref[0, piece, pl.ds(0, group * KVH)] = jnp.zeros((group * KVH, sub, HD), ref.dtype)
            store_lse(ref.at[0, piece], empty_lse)

    def own_lse(dest, piece):
        value = empty_lse
        for spot in range(group):
            latest = last_tab[piece * group + spot]
            value = jnp.where(lane_tile == spot, accl[latest, dest], value)
        return value

    def own_part(dest, piece, spot, head):
        return acc[last_tab[piece * group + spot], dest, head].astype(jnp.float32)

    def combine(values):
        peak = values[0]
        for value in values[1:]:
            peak = jnp.maximum(peak, value)
        shares = [jnp.exp(value - peak) for value in values]
        total = shares[0]
        for share in shares[1:]:
            total = total + share
        scale = 1.0 / total
        return [share * scale for share in shares], peak + jnp.log(total)

    def blend(refs, dest, piece, shares, spot, head):
        at = spot * KVH + head
        merged = shares[0][:, at : at + 1] * own_part(dest, piece, spot, head)
        for ref, share in zip(refs, shares[1:]):
            merged = merged + share[:, at : at + 1] * ref[at].astype(jnp.float32)
        return merged

    def give_partner(place, chip):
        dest = (chip % chips) * cores + (1 - core)
        for piece in range(PIECES):
            store_lse(psend.at[place, piece], own_lse(dest, piece))
            for spot in range(group):
                latest = last_tab[piece * group + spot]
                psend[place, piece, pl.ds(spot * KVH, KVH)] = acc[latest, dest]
        send(psend.at[place], precv.at[place], rs_pt_out.at[place], rs_pt.at[place], partner)

    def give_step(step):
        give_partner(step, z + ups - step)

        @pl.when(step < dns)
        def _():
            give_partner(ups + 1 + step, z + chips - dns + step)

    def hop(buf, step, place, chip, piece, out, recv, target):
        dest = (chip % chips) * cores + core

        here = buf.at[step, piece]
        theirs = precv.at[place, piece]
        local, local_lse = combine([own_lse(dest, piece), read_lse(theirs)])
        parts = [
            blend([theirs], dest, piece, local, spot, head)
            for spot in range(group)
            for head in range(KVH)
        ]

        @pl.when(step >= 1)
        def _():
            drain(here, recv.at[step - 1, piece])

        shares, lse = combine([local_lse, read_lse(here)])
        for at, part in enumerate(parts):
            arrived = shares[1][:, at : at + 1] * here[at].astype(jnp.float32)
            here[at] = (shares[0][:, at : at + 1] * part + arrived).astype(jnp.bfloat16)
        store_lse(here, lse)
        send(here, buf.at[step + 1, piece], out.at[step, piece], recv.at[step, piece], target)

    give_step(0)

    def scatter_step(step, carry):
        @pl.when(step + 1 <= ups)
        def _():
            give_step(step + 1)

        drain(precv.at[step], rs_pt.at[step])

        @pl.when(step < dns)
        def _():
            drain(precv.at[ups + 1 + step], rs_pt.at[ups + 1 + step])

        for piece in range(PIECES):
            hop(upbuf, step, step, z + ups - step, piece, rs_up_out, rs_up, above)

            @pl.when(step < dns)
            def _():
                hop(
                    dnbuf,
                    step,
                    ups + 1 + step,
                    z + chips - dns + step,
                    piece,
                    rs_dn_out,
                    rs_dn,
                    below,
                )

        return carry

    lax.fori_loop(0, ups, scatter_step, 0)
    drain(precv.at[ups], rs_pt.at[ups])
    for piece in range(PIECES):
        drain(upbuf.at[ups, piece], rs_up.at[ups - 1, piece])
        drain(dnbuf.at[dns, piece], rs_dn.at[dns - 1, piece])
        refs = [upbuf.at[ups, piece], dnbuf.at[dns, piece], precv.at[ups, piece]]
        shares, _ = combine([own_lse(me, piece)] + [read_lse(ref) for ref in refs])
        for spot in range(group):
            for head in range(KVH):
                base = ((piece * group + spot) * KVH + head) * sub
                merged = blend(refs, me, piece, shares, spot, head)
                xbuf[pl.ds(base, sub)] = merged.astype(jnp.bfloat16).astype(jnp.float32)
    for row in range(sub // GRP):
        for head in range(QH):
            first = (head // GRP) * sub + row * GRP + head % GRP
            picked = xbuf[pl.ds(first, tiles, stride=KVH * sub)]
            out_ref[pl.ds(row * tiles, tiles), head * HD : (head + 1) * HD] = picked.astype(
                jnp.bfloat16
            )

    def left(step, carry):
        for piece in range(PIECES):
            gone(upbuf.at[step, piece], rs_up_out.at[step, piece])

            @pl.when(step < dns)
            def _():
                gone(dnbuf.at[step, piece], rs_dn_out.at[step, piece])

        return carry

    lax.fori_loop(0, ups, left, 0)

    def left_partner(chip, carry):
        gone(psend.at[chip], rs_pt_out.at[chip])
        return carry

    lax.fori_loop(0, chips, left_partner, 0)


def on_device(cores, queries, keys, values, out_weight, chosen, tile_start):
    n_dev = lax.axis_size("blk")
    local_rows, tiles, width = queries.shape
    per_device = keys.shape[0] // BLOCK
    slots = per_device * CAP
    sub = local_rows * GRP
    chips = n_dev // cores
    ups = chips // 2
    dns = chips - 1 - ups
    slabs = tiles // PIECES * KVH + 1
    shards = queries.reshape(local_rows, tiles, KVH, GRP, HD)
    shards = jnp.transpose(shards, (1, 2, 0, 3, 4)).reshape(tiles, KVH, sub, HD)
    half = jnp.bfloat16
    wide = jnp.float32

    def rings(pieces):
        return [
            pltpu.SemaphoreType.DMA((ups, pieces)),
            pltpu.SemaphoreType.DMA((ups, pieces)),
            pltpu.SemaphoreType.DMA((dns, pieces)),
            pltpu.SemaphoreType.DMA((dns, pieces)),
            pltpu.SemaphoreType.DMA((chips,)),
            pltpu.SemaphoreType.DMA((chips,)),
        ]

    in_smem = pl.BlockSpec(memory_space=pltpu.SMEM)
    in_vmem = pl.BlockSpec(memory_space=pltpu.VMEM)
    anywhere = pl.BlockSpec(memory_space=pl.ANY)
    gathered_shape = (n_dev, tiles, KVH, sub, HD)
    gathered, slot_tab, last_tab = pl.pallas_call(
        functools.partial(gather_kernel, cores, per_device),
        out_shape=(
            jax.ShapeDtypeStruct(gathered_shape, half),
            jax.ShapeDtypeStruct((3, slots), jnp.int32),
            jax.ShapeDtypeStruct((tiles,), jnp.int32),
        ),
        in_specs=[in_smem, anywhere],
        out_specs=(anywhere, in_smem, in_smem),
        scratch_shapes=[
            pltpu.VMEM(gathered_shape, half),
            pltpu.SemaphoreType.DMA,
            pltpu.SemaphoreType.DMA((n_dev,)),
        ]
        + rings(SHARD_PIECES),
        compiler_params=pltpu.CompilerParams(
            collective_id=0, has_side_effects=True, vmem_limit_bytes=VMEM_LIMIT
        ),
        name="gather_queries",
    )(chosen, shards)
    acc_shape = (slots + 1, n_dev, KVH, sub, HD)
    accl_shape = (slots + 1, n_dev, sub, HD)
    acc, accl = pl.pallas_call(
        visit_kernel,
        out_shape=(
            jax.ShapeDtypeStruct(acc_shape, half),
            jax.ShapeDtypeStruct(accl_shape, wide),
        ),
        grid_spec=pltpu.PrefetchScalarGridSpec(
            num_scalar_prefetch=2,
            grid=(slots,),
            in_specs=[
                pl.BlockSpec((n_dev, 1, KVH, sub, HD), lambda s, tab, start: (0, tab[0, s], 0, 0, 0)),
                pl.BlockSpec((BLOCK, KVH * HD), lambda s, tab, start: (s // CAP, 0)),
                pl.BlockSpec((BLOCK, KVH * HD), lambda s, tab, start: (s // CAP, 0)),
            ],
            out_specs=[
                pl.BlockSpec(acc_shape, lambda s, tab, start: (0, 0, 0, 0, 0)),
                pl.BlockSpec(accl_shape, lambda s, tab, start: (0, 0, 0, 0)),
            ],
        ),
        compiler_params=pltpu.CompilerParams(
            dimension_semantics=("arbitrary",), vmem_limit_bytes=VMEM_LIMIT
        ),
        name="visits",
    )(slot_tab, tile_start, gathered, keys, values)
    merged = pl.pallas_call(
        functools.partial(scatter_kernel, cores, tiles),
        out_shape=jax.ShapeDtypeStruct((local_rows * tiles, width), half),
        in_specs=[in_smem, in_vmem, in_vmem],
        out_specs=in_vmem,
        scratch_shapes=[
            pltpu.VMEM((ups + 1, PIECES, slabs, sub, HD), half),
            pltpu.VMEM((dns + 1, PIECES, slabs, sub, HD), half),
            pltpu.VMEM((chips, PIECES, slabs, sub, HD), half),
            pltpu.VMEM((chips, PIECES, slabs, sub, HD), half),
            pltpu.VMEM((tiles * KVH * sub, HD), wide),
        ]
        + rings(PIECES),
        compiler_params=pltpu.CompilerParams(
            collective_id=1, has_side_effects=True, vmem_limit_bytes=VMEM_LIMIT
        ),
        name="merge_partials",
    )(last_tab, acc, accl)
    result = jnp.dot(merged, out_weight, preferred_element_type=jnp.float32).astype(jnp.bfloat16)
    return result.reshape(local_rows, tiles, out_weight.shape[1])


def solution(mesh):
    placed = (
        P("blk", "groups", None),
        P(("groups", "blk"), None),
        P(("groups", "blk"), None),
        P(),
        P("groups", None),
        P("groups"),
    )
    return jax.shard_map(
        functools.partial(on_device, 2),
        mesh=mesh,
        in_specs=placed,
        out_specs=P("blk", "groups", None),
        check_vma=False,
    )
```

```python
import functools
import math

import jax
import jax.numpy as jnp
from jax import lax
from jax.experimental import pallas as pl
from jax.experimental.pallas import tpu as pltpu
from jax.sharding import PartitionSpec as P

QH = 16
KVH = 4
GRP = QH // KVH
HD = 128
BLOCK = 512
CAP = 2
PIECES = 4
TERMS = 3
CHUNK_ROWS = 256
MIB = 1024 * 1024

MESH = pl.DeviceIdType.MESH
neg_big = -1e30


class Ring:
    def __init__(self, n_dev, cores):
        self.cores = cores
        self.chips = n_dev // cores
        self.ups = self.chips // 2
        self.dns = self.chips - 1 - self.ups
        me = lax.axis_index("blk")
        self.me, self.z, self.core = me, me // cores, me % cores
        self.partner = self.z * cores + (1 - self.core)
        self.above = ((self.z + 1) % self.chips) * cores + self.core
        self.below = ((self.z + self.chips - 1) % self.chips) * cores + self.core

    def greet(self):
        barrier = pltpu.get_barrier_semaphore()
        for target in (self.above, self.below, self.partner):
            pl.semaphore_signal(barrier, inc=1, device_id={"blk": target}, device_id_type=MESH)
        pl.semaphore_wait(barrier, 3)


def remote(src, dst, send_sem, recv_sem, target):
    return pltpu.make_async_remote_copy(
        src_ref=src,
        dst_ref=dst,
        send_sem=send_sem,
        recv_sem=recv_sem,
        device_id={"blk": target},
        device_id_type=MESH,
    )


def send(src, dst, send_sem, recv_sem, target):
    remote(src, dst, send_sem, recv_sem, target).start()


def gather_kernel(
    cores,
    per_device,
    chosen_ref,
    q_hbm,
    all_hbm,
    slot_tab,
    last_tab,
    gath,
    own_sem,
    store_sem,
    ag_up_out,
    ag_up,
    ag_dn_out,
    ag_dn,
    ag_pt_out,
    ag_pt,
):
    n_dev, tiles, _, sub, _ = gath.shape
    slots = per_device * CAP
    group = tiles // PIECES
    topk = chosen_ref.shape[1]
    ring = Ring(n_dev, cores)
    chips, ups, dns, cores = ring.chips, ring.ups, ring.dns, ring.cores
    me, z, core = ring.me, ring.z, ring.core
    above, below, partner = ring.above, ring.below, ring.partner

    def drain(ref, sem):
        remote(ref, ref, sem, sem, partner).wait_recv()

    def gone(ref, sem):
        remote(ref, ref, sem, sem, partner).wait_send()

    own_load = pltpu.make_async_copy(q_hbm, gath.at[me], own_sem)
    own_load.start()
    ring.greet()
    own_load.wait()

    def shard(index, piece):
        return gath.at[index, pl.ds(piece * group, group)]

    def to_partner(index):
        part = gath.at[index]
        send(part, part, ag_pt_out.at[index // cores], ag_pt.at[index // cores], partner)

    def gather_step(step, carry):
        from_below = ((z - step + chips) % chips) * cores + core
        from_above = ((z + step) % chips) * cores + core
        for piece in range(PIECES):
            part = shard(from_below, piece)

            @pl.when(step >= 1)
            def _():
                drain(part, ag_up.at[step - 1, piece])

            send(part, part, ag_up_out.at[step, piece], ag_up.at[step, piece], above)

            @pl.when(step < dns)
            def _():
                other = shard(from_above, piece)

                @pl.when(step >= 1)
                def _():
                    drain(other, ag_dn.at[step - 1, piece])

                send(other, other, ag_dn_out.at[step, piece], ag_dn.at[step, piece], below)

        to_partner(from_below)

        @pl.when((step >= 1) & (step < dns))
        def _():
            to_partner(from_above)

        return carry

    lax.fori_loop(0, ups, gather_step, 0)

    def scan_tile(tile, carry):
        firsts, lasts = carry
        new_firsts, new_lasts = [], []
        for block in range(per_device):
            hit = chosen_ref[tile, 0] == me * per_device + block
            for pick in range(1, topk):
                hit = hit | (chosen_ref[tile, pick] == me * per_device + block)
            fresh = hit & (firsts[block] == tiles)
            new_firsts.append(jnp.where(fresh, tile, firsts[block]))
            new_lasts.append(jnp.where(hit, tile, lasts[block]))
        return tuple(new_firsts), tuple(new_lasts)

    none_yet = (jnp.int32(tiles),) * per_device, (jnp.int32(-1),) * per_device
    firsts, lasts = lax.fori_loop(0, tiles, scan_tile, none_yet)
    slot_tile, slot_live = [], []
    for block in range(per_device):
        live = firsts[block] < tiles
        twice = lasts[block] > firsts[block]
        slot_tile += [jnp.where(live, firsts[block], 0), jnp.where(twice, lasts[block], 0)]
        slot_live += [live, twice]
    for slot in range(slots):
        previous = jnp.int32(slots)
        for before in range(slot):
            same = slot_live[before] & slot_live[slot] & (slot_tile[before] == slot_tile[slot])
            previous = jnp.where(same, before, previous)
        slot_tab[0, slot] = slot_tile[slot]
        slot_tab[1, slot] = jnp.where(slot_live[slot], 1, 0)
        slot_tab[2, slot] = previous
    for tile in range(tiles):
        latest = jnp.int32(slots)
        for slot in range(slots):
            latest = jnp.where(slot_live[slot] & (slot_tile[slot] == tile), slot, latest)
        last_tab[tile] = latest

    from_below = ((z - ups + chips) % chips) * cores + core
    from_above = ((z + dns) % chips) * cores + core
    for piece in range(PIECES):
        drain(shard(from_below, piece), ag_up.at[ups - 1, piece])
    to_partner(from_below)
    for piece in range(PIECES):
        drain(shard(from_above, piece), ag_dn.at[dns - 1, piece])
    to_partner(from_above)

    def partner_shard(chip, carry):
        drain(gath.at[chip * cores + (1 - core)], ag_pt.at[chip])
        for index in (chip * cores + core, chip * cores + (1 - core)):
            pltpu.make_async_copy(gath.at[index], all_hbm.at[index], store_sem.at[index]).start()
        return carry

    lax.fori_loop(0, chips, partner_shard, 0)
    def left(step, carry):
        for piece in range(PIECES):
            gone(shard(((z - step + chips) % chips) * cores + core, piece), ag_up_out.at[step, piece])

            @pl.when(step < dns)
            def _():
                gone(shard(((z + step) % chips) * cores + core, piece), ag_dn_out.at[step, piece])

        return carry

    lax.fori_loop(0, ups, left, 0)

    def left_partner(chip, carry):
        gone(gath.at[chip * cores + core], ag_pt_out.at[chip])
        return carry

    lax.fori_loop(0, chips, left_partner, 0)

    def stored(index, carry):
        pltpu.make_async_copy(gath.at[index], all_hbm.at[index], store_sem.at[index]).wait()
        return carry

    lax.fori_loop(0, n_dev, stored, 0)


def visit_kernel(slot_tab, start_ref, q_ref, k_ref, v_ref, acc, accl):
    slot = pl.program_id(0)
    slots = pl.num_programs(0)
    n_dev, _, _, sub, _ = q_ref.shape
    rows = n_dev * sub
    chunk_rows = min(CHUNK_ROWS, rows)
    chunk_devs = chunk_rows // sub
    chunks = rows // chunk_rows
    per_device = slots // CAP
    block = slot // CAP
    tile = slot_tab[0, slot]
    previous = slot_tab[2, slot]
    offset = start_ref[tile] - (lax.axis_index("blk") * per_device + block) * BLOCK

    @pl.when(slot == 0)
    def _():
        acc[slots] = jnp.zeros(acc.shape[1:], acc.dtype)
        accl[slots] = jnp.full(accl.shape[1:], neg_big, accl.dtype)

    @pl.when(slot_tab[1, slot] > 0)
    def _():
        def visit(chunk, masked):
            devs = pl.ds(chunk * chunk_devs, chunk_devs)
            if masked:
                row = lax.broadcasted_iota(jnp.int32, (chunk_rows, BLOCK), 0) + chunk * chunk_rows
                ahead = lax.broadcasted_iota(jnp.int32, (chunk_rows, BLOCK), 1) - row // GRP
                visible = ahead <= offset
            wide = lax.broadcasted_iota(jnp.int32, (chunk_rows, HD), 1) % KVH
            before_lse = accl[previous, devs].reshape(chunk_rows, HD)
            packed = jnp.zeros((chunk_rows, HD), jnp.float32)
            for head in range(KVH):
                query = q_ref[devs, 0, head].astype(jnp.float32)
                query = query.reshape(chunk_rows, HD).astype(jnp.bfloat16)
                key = k_ref[:, head * HD : (head + 1) * HD]
                value = v_ref[:, head * HD : (head + 1) * HD]
                scores = lax.dot_general(
                    query, key, (((1,), (1,)), ((), ())), preferred_element_type=jnp.float32
                )
                if masked:
                    scores = jnp.where(visible, scores, neg_big)
                highest = jnp.max(scores, axis=1, keepdims=True)
                weights = jnp.exp2((scores - highest) * (math.log2(math.e) / math.sqrt(HD)))
                total = jnp.sum(weights, axis=1, keepdims=True)
                weights = (weights * (1.0 / total)).astype(jnp.bfloat16)
                partial = jnp.dot(weights, value, preferred_element_type=jnp.float32)
                partial = partial.astype(jnp.bfloat16).astype(jnp.float32)
                lse = highest * (1.0 / math.sqrt(HD)) + jnp.log(total)
                old_lse = before_lse[:, head : head + 1]
                old = acc[previous, devs, head].astype(jnp.float32).reshape(chunk_rows, HD)
                peak = jnp.maximum(lse, old_lse)
                new_part = jnp.exp(lse - peak)
                old_part = jnp.exp(old_lse - peak)
                both = new_part + old_part
                scale = 1.0 / both
                partial = (new_part * scale) * partial + (old_part * scale) * old
                acc[slot, devs, head] = partial.reshape(chunk_devs, sub, HD).astype(jnp.bfloat16)
                packed = jnp.where(wide == head, peak + jnp.log(both), packed)
            accl[slot, devs] = packed.reshape(chunk_devs, sub, HD)

        def visits(masked):
            def step(chunk, carry):
                visit(chunk, masked)
                return carry

            lax.fori_loop(0, chunks, step, 0)

        pl.when(offset >= BLOCK - 1)(lambda: visits(False))
        pl.when(offset < BLOCK - 1)(lambda: visits(True))


def scatter_kernel(
    cores,
    tiles,
    last_tab,
    acc,
    accl,
    out_ref,
    upbuf,
    dnbuf,
    psend,
    precv,
    xbuf,
    rs_up_out,
    rs_up,
    rs_dn_out,
    rs_dn,
    rs_pt_out,
    rs_pt,
):
    _, n_dev, _, sub, _ = acc.shape
    group = tiles // PIECES
    ring = Ring(n_dev, cores)
    chips, ups, dns, cores = ring.chips, ring.ups, ring.dns, ring.cores
    me, z, core = ring.me, ring.z, ring.core
    above, below, partner = ring.above, ring.below, ring.partner

    def drain(ref, sem):
        remote(ref, ref, sem, sem, partner).wait_recv()

    def gone(ref, sem):
        remote(ref, ref, sem, sem, partner).wait_send()

    ring.greet()
    lane = lax.broadcasted_iota(jnp.int32, (sub, HD), 1)
    width = group * KVH
    lane_tile = (lane % width) // KVH

    def store_lse(ref, value):
        packed = jnp.zeros_like(value)
        rest = value
        for term in range(TERMS):
            part = rest.astype(jnp.bfloat16).astype(jnp.float32)
            rest = rest - part
            here = (lane >= term * width) & (lane < (term + 1) * width)
            packed = jnp.where(here, pltpu.roll(part, term * width, 1) if term else part, packed)
        ref[group * KVH] = packed.astype(jnp.bfloat16)

    def read_lse(ref):
        packed = ref[group * KVH].astype(jnp.float32)
        total = packed
        for term in range(1, TERMS):
            total = total + pltpu.roll(packed, HD - term * width, 1)
        return total

    empty_lse = jnp.full((sub, HD), neg_big, jnp.float32)
    for ref in (upbuf, dnbuf):
        for piece in range(PIECES):
            ref[0, piece, pl.ds(0, group * KVH)] = jnp.zeros((group * KVH, sub, HD), ref.dtype)
            store_lse(ref.at[0, piece], empty_lse)

    def own_lse(dest, piece):
        value = empty_lse
        for spot in range(group):
            latest = last_tab[piece * group + spot]
            value = jnp.where(lane_tile == spot, accl[latest, dest], value)
        return value

    def own_part(dest, piece, spot, head):
        return acc[last_tab[piece * group + spot], dest, head].astype(jnp.float32)

    def combine(values):
        peak = values[0]
        for value in values[1:]:
            peak = jnp.maximum(peak, value)
        shares = [jnp.exp(value - peak) for value in values]
        total = shares[0]
        for share in shares[1:]:
            total = total + share
        scale = 1.0 / total
        return [share * scale for share in shares], peak + jnp.log(total)

    def blend(refs, dest, piece, shares, spot, head):
        at = spot * KVH + head
        merged = shares[0][:, at : at + 1] * own_part(dest, piece, spot, head)
        for ref, share in zip(refs, shares[1:]):
            merged = merged + share[:, at : at + 1] * ref[at].astype(jnp.float32)
        return merged.astype(jnp.bfloat16)

    def give_partner(place, chip):
        dest = (chip % chips) * cores + (1 - core)
        for piece in range(PIECES):
            store_lse(psend.at[place, piece], own_lse(dest, piece))
            for spot in range(group):
                latest = last_tab[piece * group + spot]
                psend[place, piece, pl.ds(spot * KVH, KVH)] = acc[latest, dest]
        send(psend.at[place], precv.at[place], rs_pt_out.at[place], rs_pt.at[place], partner)

    def give_step(step):
        give_partner(step, z + ups - step)

        @pl.when(step < dns)
        def _():
            give_partner(ups + 1 + step, z + chips - dns + step)

    def hop(buf, step, place, chip, piece, out, recv, target):
        dest = (chip % chips) * cores + core

        @pl.when(step >= 1)
        def _():
            drain(buf.at[step, piece], recv.at[step - 1, piece])

        here = buf.at[step, piece]
        theirs = precv.at[place, piece]
        shares, lse = combine([own_lse(dest, piece), read_lse(here), read_lse(theirs)])
        for spot in range(group):
            for head in range(KVH):
                here[spot * KVH + head] = blend([here, theirs], dest, piece, shares, spot, head)
        store_lse(here, lse)
        send(here, buf.at[step + 1, piece], out.at[step, piece], recv.at[step, piece], target)

    give_step(0)

    def scatter_step(step, carry):
        @pl.when(step + 1 <= ups)
        def _():
            give_step(step + 1)

        drain(precv.at[step], rs_pt.at[step])

        @pl.when(step < dns)
        def _():
            drain(precv.at[ups + 1 + step], rs_pt.at[ups + 1 + step])

        for piece in range(PIECES):
            hop(upbuf, step, step, z + ups - step, piece, rs_up_out, rs_up, above)

            @pl.when(step < dns)
            def _():
                hop(
                    dnbuf,
                    step,
                    ups + 1 + step,
                    z + chips - dns + step,
                    piece,
                    rs_dn_out,
                    rs_dn,
                    below,
                )

        return carry

    lax.fori_loop(0, ups, scatter_step, 0)
    drain(precv.at[ups], rs_pt.at[ups])
    for piece in range(PIECES):
        drain(upbuf.at[ups, piece], rs_up.at[ups - 1, piece])
        drain(dnbuf.at[dns, piece], rs_dn.at[dns - 1, piece])
        refs = [upbuf.at[ups, piece], dnbuf.at[dns, piece], precv.at[ups, piece]]
        shares, _ = combine([own_lse(me, piece)] + [read_lse(ref) for ref in refs])
        for spot in range(group):
            for head in range(KVH):
                base = ((piece * group + spot) * KVH + head) * sub
                merged = blend(refs, me, piece, shares, spot, head)
                xbuf[pl.ds(base, sub)] = merged.astype(jnp.float32)
    for row in range(sub // GRP):
        for head in range(QH):
            first = (head // GRP) * sub + row * GRP + head % GRP
            picked = xbuf[pl.ds(first, tiles, stride=KVH * sub)]
            out_ref[pl.ds(row * tiles, tiles), head * HD : (head + 1) * HD] = picked.astype(
                jnp.bfloat16
            )

    def left(step, carry):
        for piece in range(PIECES):
            gone(upbuf.at[step, piece], rs_up_out.at[step, piece])

            @pl.when(step < dns)
            def _():
                gone(dnbuf.at[step, piece], rs_dn_out.at[step, piece])

        return carry

    lax.fori_loop(0, ups, left, 0)

    def left_partner(chip, carry):
        gone(psend.at[chip], rs_pt_out.at[chip])
        return carry

    lax.fori_loop(0, chips, left_partner, 0)


def on_device(cores, queries, keys, values, out_weight, chosen, tile_start):
    n_dev = lax.axis_size("blk")
    local_rows, tiles, width = queries.shape
    per_device = keys.shape[0] // BLOCK
    slots = per_device * CAP
    sub = local_rows * GRP
    chips = n_dev // cores
    ups = chips // 2
    dns = chips - 1 - ups
    slabs = tiles // PIECES * KVH + 1
    shards = queries.reshape(local_rows, tiles, KVH, GRP, HD)
    shards = jnp.transpose(shards, (1, 2, 0, 3, 4)).reshape(tiles, KVH, sub, HD)
    half = jnp.bfloat16
    wide = jnp.float32
    rings = [
        pltpu.SemaphoreType.DMA((ups, PIECES)),
        pltpu.SemaphoreType.DMA((ups, PIECES)),
        pltpu.SemaphoreType.DMA((dns, PIECES)),
        pltpu.SemaphoreType.DMA((dns, PIECES)),
        pltpu.SemaphoreType.DMA((chips,)),
        pltpu.SemaphoreType.DMA((chips,)),
    ]
    in_smem = pl.BlockSpec(memory_space=pltpu.SMEM)
    in_vmem = pl.BlockSpec(memory_space=pltpu.VMEM)
    anywhere = pl.BlockSpec(memory_space=pl.ANY)
    gathered_shape = (n_dev, tiles, KVH, sub, HD)
    gathered, slot_tab, last_tab = pl.pallas_call(
        functools.partial(gather_kernel, cores, per_device),
        out_shape=(
            jax.ShapeDtypeStruct(gathered_shape, half),
            jax.ShapeDtypeStruct((3, slots), jnp.int32),
            jax.ShapeDtypeStruct((tiles,), jnp.int32),
        ),
        in_specs=[in_smem, anywhere],
        out_specs=(anywhere, in_smem, in_smem),
        scratch_shapes=[
            pltpu.VMEM(gathered_shape, half),
            pltpu.SemaphoreType.DMA,
            pltpu.SemaphoreType.DMA((n_dev,)),
        ]
        + rings,
        compiler_params=pltpu.CompilerParams(
            collective_id=0, has_side_effects=True, vmem_limit_bytes=24 * MIB
        ),
        name="gather_queries",
    )(chosen, shards)
    acc_shape = (slots + 1, n_dev, KVH, sub, HD)
    accl_shape = (slots + 1, n_dev, sub, HD)
    acc, accl = pl.pallas_call(
        visit_kernel,
        out_shape=(
            jax.ShapeDtypeStruct(acc_shape, half),
            jax.ShapeDtypeStruct(accl_shape, wide),
        ),
        grid_spec=pltpu.PrefetchScalarGridSpec(
            num_scalar_prefetch=2,
            grid=(slots,),
            in_specs=[
                pl.BlockSpec((n_dev, 1, KVH, sub, HD), lambda s, tab, start: (0, tab[0, s], 0, 0, 0)),
                pl.BlockSpec((BLOCK, KVH * HD), lambda s, tab, start: (s // CAP, 0)),
                pl.BlockSpec((BLOCK, KVH * HD), lambda s, tab, start: (s // CAP, 0)),
            ],
            out_specs=[
                pl.BlockSpec(acc_shape, lambda s, tab, start: (0, 0, 0, 0, 0)),
                pl.BlockSpec(accl_shape, lambda s, tab, start: (0, 0, 0, 0)),
            ],
        ),
        compiler_params=pltpu.CompilerParams(
            dimension_semantics=("arbitrary",), vmem_limit_bytes=32 * MIB
        ),
        name="visits",
    )(slot_tab, tile_start, gathered, keys, values)
    merged = pl.pallas_call(
        functools.partial(scatter_kernel, cores, tiles),
        out_shape=jax.ShapeDtypeStruct((local_rows * tiles, width), half),
        in_specs=[in_smem, in_vmem, in_vmem],
        out_specs=in_vmem,
        scratch_shapes=[
            pltpu.VMEM((ups + 1, PIECES, slabs, sub, HD), half),
            pltpu.VMEM((dns + 1, PIECES, slabs, sub, HD), half),
            pltpu.VMEM((chips, PIECES, slabs, sub, HD), half),
            pltpu.VMEM((chips, PIECES, slabs, sub, HD), half),
            pltpu.VMEM((tiles * KVH * sub, HD), wide),
        ]
        + rings,
        compiler_params=pltpu.CompilerParams(
            collective_id=1, has_side_effects=True, vmem_limit_bytes=36 * MIB
        ),
        name="merge_partials",
    )(last_tab, acc, accl)
    result = jnp.dot(merged, out_weight, preferred_element_type=jnp.float32).astype(jnp.bfloat16)
    return result.reshape(local_rows, tiles, out_weight.shape[1])


def solution(mesh):
    placed = (
        P("blk", "groups", None),
        P(("groups", "blk"), None),
        P(("groups", "blk"), None),
        P(),
        P("groups", None),
        P("groups"),
    )
    return jax.shard_map(
        functools.partial(on_device, 2),
        mesh=mesh,
        in_specs=placed,
        out_specs=P("blk", "groups", None),
        check_vma=False,
    )
```
